32 devices in a mesh: groups: 2 (over x), win: 16 (over z, y, core).
Axes of the slice: x: 2, y: 2, z: 4, core: 2. Of those that a mesh axis runs over, the one named last changes fastest.
Arguments:
- latents: bfloat16 [6, 8, 256, 1536], P('groups', None, 'win'), parts along dimension 0, may hold values from -60 to 60
- offsets: int32 [6], P('groups'), parts along dimension 0, may hold values from 0 to 8, as said below
- levels: int32 [6], P('groups'), parts along dimension 0, may hold values from 0 to 31
- mod_table: bfloat16 [32, 6, 1536], replicated, may hold values from -3 to 3
- rel_bias: float32 [6, 64, 64], replicated, may hold values from -3 to 403
- w_qkv: bfloat16 [1536, 2304], P('win'), may hold values from -0.15625 to 0.15625
- w_out: bfloat16 [768, 1536], P('win'), may hold values from -0.21875 to 0.21875
- w_up: bfloat16 [1536, 3072], P('win'), may hold values from -0.15625 to 0.15625
- w_down: bfloat16 [3072, 1536], P('win'), may hold values from -0.109375 to 0.109375
Outputs:
- result: bfloat16 [6, 8, 256, 1536], P('groups', None, 'win'), parts along dimension 0
The draws below stay inside these ranges and needn't reach their ends.
There are 2 independent parts, one for each index of `groups`. The reference program is written for one: setup_inputs(seed, part) draws one part's arguments, and reference() takes and returns one part's arrays. A program takes and returns all parts, laid end to end along the dimension named above; an argument that names none is the same for every part. Nothing has to cross between parts.
Inputs may be any that keep to these rules, and one draw needn't show every extreme that they name: `offsets`: some micro-batch has offset 8 in every draw.
All inputs are finite; a program needn't handle non-finite values.
Results may differ from the reference program's by a relative error of at most 0.007.
Values may be sent and summed in bfloat16 or wider, within the bound.
No kernel may reach another device: no remote copies, remote signals or barrier semaphores. Data moves between devices by JAX's collectives and lax.ppermute only.
A program may use at most 128 MiB of HBM per device.

```python
import jax
import jax.numpy as jnp
from jax import lax

D = 1536
HEADS = 6
HEAD_DIM = 128
FF = 3072
WIN = 8
LEVELS = 32
MB = 3
LON = 256


def draw_latents(key, part):
    first = jax.random.fold_in(jax.random.fold_in(key, 11), 0)
    base = jax.random.normal(first, (MB, WIN, LON, D), jnp.float32)
    return jnp.clip(base, -6.0, 6.0).astype(jnp.bfloat16)


def draw_rel_bias(key, part):
    keys = jax.random.split(jax.random.fold_in(key, 23), 1)
    width = WIN * WIN
    base = jnp.clip(jax.random.normal(keys[0], (HEADS, width, width), jnp.float32), -3.0, 3.0)
    return base.astype(jnp.float32)


def draw_offsets(key, part):
    first, second = jax.random.split(jax.random.fold_in(key, 37))
    values_drawn = jax.random.randint(first, (MB,), 0, WIN + 1)
    place = jax.random.randint(second, (), 0, MB)
    return jnp.where(jnp.arange(MB, dtype=jnp.int32) == place, WIN, values_drawn).astype(jnp.int32)


def block_levels(key, dims, shards, least, top_value):
    def one(dim, blocks):
        draws = jax.random.uniform(jax.random.fold_in(jax.random.fold_in(key, 6), dim), (blocks,), jnp.float32, least / len(shards), top_value / len(shards))
        return jnp.repeat(jnp.exp(draws), dims[dim] // blocks).reshape((-1,) + (1,) * (len(dims) - dim - 1))

    level = one(*shards[0])
    for cut in shards[1:]:
        level = level * one(*cut)
    return level


def bell_draw(key, extent, scale, most, shards=(), kind=jnp.bfloat16):
    factor_of = block_levels(key, extent, shards, -0.22, 0.18) if shards else 1.0
    drawn = jax.random.normal(key, extent, jnp.float32) * scale * factor_of
    return jnp.minimum(jnp.maximum(drawn, -most), most).astype(kind)


def setup_inputs(seed: int = 0, part: int = 0) -> dict:
    splits = jax.random.split(jax.random.key(seed), 10)
    part_splits = jax.random.split(jax.random.fold_in(splits[9], part), 10)
    return {
        "latents": draw_latents(jax.random.fold_in(jax.random.fold_in(splits[9], part), 71), part),
        "offsets": draw_offsets(jax.random.fold_in(jax.random.fold_in(splits[9], part), 71), part),
        "levels": jax.random.randint(part_splits[2], (MB,), 0, LEVELS).astype(jnp.int32),
        "mod_table": bell_draw(splits[3], (LEVELS, 6, D), 0.5, 3.0),
        "rel_bias": draw_rel_bias(jax.random.fold_in(splits[9], 71), part),
        "w_qkv": bell_draw(splits[5], (D, 3 * HEADS * HEAD_DIM), D ** -0.5, 0.15625, ((0, 16),)),
        "w_out": bell_draw(splits[6], (HEADS * HEAD_DIM, D), (HEADS * HEAD_DIM) ** -0.5, 0.21875, ((0, 16),)),
        "w_up": bell_draw(splits[7], (D, FF), D ** -0.5, 0.15625, ((0, 16),)),
        "w_down": bell_draw(splits[8], (FF, D), FF ** -0.5, 0.109375, ((0, 16),)),
    }


def norm_rows(values_in):
    centre = values_in - lax.optimization_barrier(jnp.mean(values_in, axis=-1, keepdims=True))
    spread = lax.optimization_barrier(jnp.mean(centre * centre, axis=-1, keepdims=True))
    return centre * lax.rsqrt(spread + 1e-06)

def reference(latents, offsets, levels, mod_table, rel_bias, w_qkv, w_out, w_up, w_down):
    batches, lat_rows, columns, features = latents.shape
    inner = HEADS * HEAD_DIM
    selector = (levels[:, None] == jnp.arange(LEVELS, dtype=jnp.int32)[None, :]).astype(jnp.float32)
    modulation = jnp.einsum('ml,lkd->mkd', selector, mod_table.astype(jnp.float32))
    modulation = modulation.reshape(batches, 6, 1, 1, features)
    stream = latents.astype(jnp.float32)
    normed = (norm_rows(stream) * (1.0 + modulation[:, 0]) + modulation[:, 1]).astype(jnp.bfloat16)
    rolled = jax.vmap(lambda region, shift_by: jnp.roll(region, shift_by, axis=1))(normed, offsets)
    per_row = columns // WIN
    windows = rolled.reshape(batches, lat_rows, per_row, WIN, features).transpose(0, 2, 1, 3, 4)
    windows = windows.reshape(-1, lat_rows * WIN, features)
    number = windows.shape[0]
    triple = jnp.dot(windows.reshape(-1, features), w_qkv, preferred_element_type=jnp.float32)
    triple = triple.astype(jnp.bfloat16).reshape(number, lat_rows * WIN, 3, HEADS, HEAD_DIM)
    triple = triple.astype(jnp.float32)
    scores = jnp.einsum('wqhe,wkhe->whqk', triple[:, :, 0], triple[:, :, 1]) * (1.0 / HEAD_DIM ** 0.5)
    scores = scores + rel_bias[None]
    probs = jax.nn.softmax(scores, axis=-1).astype(jnp.bfloat16)
    attended = jnp.einsum('whqk,wkhe->wqhe', probs.astype(jnp.float32), triple[:, :, 2]).astype(jnp.bfloat16)
    projected = jnp.dot(attended.reshape(-1, inner), w_out, preferred_element_type=jnp.float32)
    projected = projected.reshape(batches, per_row, lat_rows, WIN, features).transpose(0, 2, 1, 3, 4)
    projected = projected.reshape(batches, lat_rows, columns, features)
    projected = jax.vmap(lambda region, shift_by: jnp.roll(region, -shift_by, axis=1))(projected, offsets)
    middle = (stream + modulation[:, 2] * projected).astype(jnp.bfloat16)
    second = (norm_rows(middle.astype(jnp.float32)) * (1.0 + modulation[:, 3]) + modulation[:, 4]).astype(jnp.bfloat16)
    hidden = jnp.dot(second.reshape(-1, features), w_up, preferred_element_type=jnp.float32)
    hidden = jax.nn.gelu(hidden, approximate=False).astype(jnp.bfloat16)
    lowered = jnp.dot(hidden, w_down, preferred_element_type=jnp.float32).reshape(batches, lat_rows, columns, features)
    return (middle.astype(jnp.float32) + modulation[:, 5] * lowered).astype(jnp.bfloat16)
```

```python
import functools

import jax
import jax.numpy as jnp
from jax import lax
from jax.experimental import pallas as pl
from jax.experimental.pallas import tpu as pltpu
from jax.sharding import PartitionSpec as P

HEADS = 6
HEAD_DIM = 128
WIN = 8
LEVELS = 32


def passed_along(shard, axis, by):
    length = lax.axis_size(axis)
    return lax.ppermute(shard, axis, [(i, (i + by) % length) for i in range(length)])


def norm_rows(values_in):
    centre = values_in - jnp.mean(values_in, axis=-1, keepdims=True)
    spread = jnp.mean(centre * centre, axis=-1, keepdims=True)
    return centre * lax.rsqrt(spread + 1e-06)


def restore_grid(region, arrived, offsets, columns):
    widened = jnp.concatenate([region, arrived], axis=2)
    return jax.vmap(lambda plane, shift_by: lax.dynamic_slice_in_dim(plane, shift_by, columns, 1))(
        widened, offsets
    )


def plain(latents, offsets, levels, mod_table, rel_bias, w_qkv, w_out, w_up, w_down):
    batches, lat_rows, columns, features = latents.shape
    inner = HEADS * HEAD_DIM
    per_dev = columns // WIN
    selector = (levels[:, None] == jnp.arange(LEVELS, dtype=jnp.int32)[None, :]).astype(
        jnp.bfloat16
    )
    modulation = jnp.dot(
        selector, mod_table.reshape(LEVELS, 6 * features), preferred_element_type=jnp.float32
    )
    modulation = modulation.reshape(batches, 6, 1, 1, features)
    stream = latents.astype(jnp.float32)
    normed = (norm_rows(stream) * (1.0 + modulation[:, 0]) + modulation[:, 1]).astype(jnp.bfloat16)
    arrived = passed_along(normed[:, :, columns - WIN :, :], "win", 1)
    widened = jnp.concatenate([arrived, normed], axis=2)
    rolled = jax.vmap(
        lambda plane, shift_by: lax.dynamic_slice_in_dim(plane, WIN - shift_by, columns, 1)
    )(widened, offsets)
    full_qkv = lax.all_gather(w_qkv, "win", axis=0, tiled=True)
    windows = rolled.reshape(batches, lat_rows, per_dev, WIN, features).transpose(0, 2, 1, 3, 4)
    windows = windows.reshape(-1, lat_rows * WIN, features)
    number = windows.shape[0]
    triple = jnp.dot(windows.reshape(-1, features), full_qkv, preferred_element_type=jnp.float32)
    triple = triple.astype(jnp.bfloat16).reshape(number, lat_rows * WIN, 3, HEADS, HEAD_DIM)
    scores = jnp.einsum(
        "wqhe,wkhe->whqk", triple[:, :, 0], triple[:, :, 1], preferred_element_type=jnp.float32
    )
    scores = scores * (1.0 / HEAD_DIM**0.5) + rel_bias[None]
    probs = jax.nn.softmax(scores, axis=-1).astype(jnp.bfloat16)
    attended = jnp.einsum(
        "whqk,wkhe->wqhe", probs, triple[:, :, 2], preferred_element_type=jnp.float32
    ).astype(jnp.bfloat16)
    attended = attended.reshape(batches, per_dev, lat_rows, WIN, inner).transpose(0, 2, 1, 3, 4)
    attended = attended.reshape(batches, lat_rows, columns, inner)
    full_out = lax.all_gather(w_out, "win", axis=0, tiled=True)
    returned = passed_along(attended[:, :, :WIN, :], "win", -1)
    restored = restore_grid(attended, returned, offsets, columns)
    projected = jnp.dot(restored.reshape(-1, inner), full_out, preferred_element_type=jnp.float32)
    projected = projected.reshape(batches, lat_rows, columns, features)
    middle = (stream + modulation[:, 2] * projected).astype(jnp.bfloat16)
    second = (
        norm_rows(middle.astype(jnp.float32)) * (1.0 + modulation[:, 3]) + modulation[:, 4]
    ).astype(jnp.bfloat16)
    full_up = lax.all_gather(w_up, "win", axis=0, tiled=True)
    hidden = jnp.dot(second.reshape(-1, features), full_up, preferred_element_type=jnp.float32)
    hidden = jax.nn.gelu(hidden, approximate=False).astype(jnp.bfloat16)
    full_down = lax.all_gather(w_down, "win", axis=0, tiled=True)
    lowered = jnp.dot(hidden, full_down, preferred_element_type=jnp.float32).reshape(
        batches, lat_rows, columns, features
    )
    return (middle.astype(jnp.float32) + modulation[:, 5] * lowered).astype(jnp.bfloat16)


AXES = ("groups", "win")


class Ring:
    def __init__(self, mesh):
        self.groups, self.length = mesh.shape["groups"], mesh.shape["win"]
        places = [tuple(d.coords) for d in mesh.devices.reshape(self.groups, self.length)[0]]
        self.ys = len({p[1] for p in places})
        self.zs = self.length // (2 * self.ys)

    def place(self, win):
        return win // (2 * self.ys), win // 2 % self.ys, win % 2

    def index(self, z, y, core):
        return (z % self.zs * self.ys + y % self.ys) * 2 + core

    def pairs(self, dx=0, dz=0, dy=0, dcore=0):
        out = []
        for group in range(self.groups):
            for win in range(self.length):
                z, y, core = self.place(win)
                target = self.index(z + dz, y + dy, (core + dcore) % 2)
                out.append((group * self.length + win, (group + dx) % self.groups * self.length + target))
        return out

    def fits(self, w_qkv, w_out, w_up, w_down):
        rows = w_up.shape[0] // self.length
        features, ff = w_up.shape
        return (
            self.groups == 2
            and self.ys == 2
            and self.zs == 4
            and rows % 96 == 0
            and w_out.shape[0] * 2 == features
            and ff == 2 * features
            and w_qkv.shape[1] * 2 == 3 * features
        )


def moved(block, pairs):
    return lax.ppermute(block, AXES, pairs)


def gathered(ring, third, core_groups):
    pieces = {"r1": moved(third, ring.pairs(dz=1)), "y0": moved(third, ring.pairs(dy=1))}
    pieces["r2"] = moved(pieces["r1"], ring.pairs(dz=1))
    pieces["y1"] = moved(pieces["r1"], ring.pairs(dy=1))
    pieces["r3"] = moved(pieces["r2"], ring.pairs(dz=1))
    pieces["y2"] = moved(pieces["r2"], ring.pairs(dy=1))
    pieces["y3"] = moved(pieces["r3"], ring.pairs(dy=1))
    half = third.shape[0] // 2
    crossing = {"x1": ("r1", "y0"), "x2": ("r2", "y1"), "x3": ("r3", "y2"), "x4": ("y3",)}
    for name, members in crossing.items():
        block = [pieces[member][:half] for member in members]
        block = jnp.concatenate(block, axis=0) if len(block) > 1 else block[0]
        pieces[name] = moved(block, ring.pairs(dx=1))
    place, buffers = {}, []
    for name, piece in pieces.items():
        place["mine", name] = (len(buffers), 0)
        buffers.append(piece)
    for members in core_groups:
        block = [pieces[member] for member in members]
        block = jnp.concatenate(block, axis=0) if len(block) > 1 else block[0]
        at = 0
        for member in members:
            place["other", member] = (len(buffers), at)
            at += pieces[member].shape[0]
        buffers.append(moved(block, ring.pairs(dcore=1)))
    sources = {}
    for side in ("mine", "other"):
        for slot, name in enumerate(("r1", "r2", "r3", "y0", "y1", "y2", "y3")):
            buffer, at = place[side, name]
            crossed = next(x for x, members in crossing.items() if name in members)
            other, back = place[side, crossed]
            back += half * crossing[crossed].index(name)
            sources[side, slot + 1] = ((buffer, at), (buffer, at + half), (other, back))
    return buffers, sources


def fetch(spec, scalars, own, other, buffers, sems):
    sources, whole, piece = spec
    copies = []

    def start(src, dst):
        copy = pltpu.make_async_copy(src, dst, sems.at[len(copies)])
        copy.start()
        copies.append(copy)

    for number, ref in ((0, own), (8, other)):
        for src, dst in whole(ref, scalars[number]):
            start(src, dst)
    here = scalars[16]
    for (side, slot), parts in sources.items():
        shard = scalars[slot + (0 if side == "mine" else 8)]
        for number, (kind, (buffer, row)) in enumerate(zip((here, 2, 1 - here), parts)):
            for src, dst in piece(buffers[buffer], row, shard, kind, number == 1):
                start(src, dst)
    return copies


def tile(value):
    return pl.multiple_of(value, 16)


def attention_kernel(sources, scalars, rolled, bias, own, other, *rest):
    buffers, (out, weight, triple, sems) = rest[:-4], rest[-4:]
    rows, features = own.shape[0], rolled.shape[1]
    heads, inner = bias.shape[0], out.shape[1]
    half = rows // 2

    def whole(ref, shard):
        yield ref, weight.at[pl.ds(tile(shard * rows), rows)]

    def piece(ref, row, shard, kind, last):
        if last:
            for side in range(2):
                yield (
                    ref.at[pl.ds(row, half), pl.ds(side * inner, inner)],
                    weight.at[pl.ds(tile(shard * rows + side * half), half), pl.ds(features, inner)],
                )
        else:
            yield (
                ref.at[pl.ds(row, half)],
                weight.at[pl.ds(tile(shard * rows + kind * half), half), pl.ds(0, features)],
            )

    copies = fetch((sources, whole, piece), scalars, own, other, buffers, sems)
    for copy in copies:
        copy.wait()
    step = 2 * HEAD_DIM

    def project(i, carry):
        at = pl.ds(pl.multiple_of(i * step, step), step)
        triple[:, at] = jnp.dot(
            rolled[...], weight[:, at], preferred_element_type=jnp.float32
        ).astype(triple.dtype)
        return carry

    lax.fori_loop(0, weight.shape[1] // step, project, 0)
    tokens = bias.shape[1]

    def window(i, carry):
        span = pl.ds(pl.multiple_of(i * tokens, tokens), tokens)
        for head in range(heads):
            cut = [triple[span, part * inner + head * HEAD_DIM : part * inner + (head + 1) * HEAD_DIM] for part in range(3)]
            scores = lax.dot_general(
                cut[0], cut[1], (((1,), (1,)), ((), ())), preferred_element_type=jnp.float32
            )
            scores = scores * (1.0 / HEAD_DIM**0.5) + bias[head]
            powers = jnp.exp(scores - jnp.max(scores, axis=-1, keepdims=True))
            probs = (powers / jnp.sum(powers, axis=-1, keepdims=True)).astype(jnp.bfloat16)
            mixed = jnp.dot(probs, cut[2], preferred_element_type=jnp.float32)
            out[span, head * HEAD_DIM : (head + 1) * HEAD_DIM] = mixed.astype(out.dtype)
        return carry

    lax.fori_loop(0, rolled.shape[0] // tokens, window, 0)


def project_kernel(sources, scalars, attended, latents, modulation, own, other, *rest):
    buffers, (middle, second, weight, sems) = rest[:-4], rest[-4:]
    rows = own.shape[0]
    part = rows // 3

    def whole(ref, shard):
        yield ref, weight.at[pl.ds(tile(shard * rows), rows)]

    def piece(ref, row, shard, kind, last):
        yield ref.at[pl.ds(row + rows, part)], weight.at[pl.ds(tile(shard * rows + kind * part), part)]

    copies = fetch((sources, whole, piece), scalars, own, other, buffers, sems)
    for copy in copies:
        copy.wait()
    batches = modulation.shape[0]
    tokens = latents.shape[0] // batches
    for batch in range(batches):
        span = slice(batch * tokens, (batch + 1) * tokens)
        projected = jnp.dot(attended[span, :], weight[...], preferred_element_type=jnp.float32)
        mod = modulation[batch]
        mixed = (latents[span, :].astype(jnp.float32) + mod[2:3] * projected).astype(middle.dtype)
        middle[span, :] = mixed
        normed = norm_rows(mixed.astype(jnp.float32)) * (1.0 + mod[3:4]) + mod[4:5]
        second[span, :] = normed.astype(second.dtype)


def up_kernel(sources, scalars, second, own, other, *rest):
    buffers, (hidden, weight, sems) = rest[:-3], rest[-3:]
    rows, features = own.shape[0], second.shape[1]
    part = rows // 3

    def whole(ref, shard):
        yield ref, weight.at[pl.ds(tile(shard * rows), rows)]

    def piece(ref, row, shard, kind, last):
        for side in range(2):
            yield (
                ref.at[pl.ds(row + side * part, part)],
                weight.at[pl.ds(tile(shard * rows + kind * part), part), pl.ds(side * features, features)],
            )

    copies = fetch((sources, whole, piece), scalars, own, other, buffers, sems)
    for copy in copies:
        copy.wait()
    step = 2 * HEAD_DIM

    def body(i, carry):
        at = pl.ds(pl.multiple_of(i * step, step), step)
        value = jnp.dot(second[...], weight[:, at], preferred_element_type=jnp.float32)
        value = 0.5 * value * (1.0 + lax.erf(value * 0.5**0.5))
        hidden[:, at] = value.astype(hidden.dtype)
        return carry

    lax.fori_loop(0, weight.shape[1] // step, body, 0)


def down_kernel(sources, scalars, hidden, middle, modulation, own, other, *rest):
    buffers, (out, weight, sems) = rest[:-3], rest[-3:]
    rows = own.shape[0]
    part = rows // 3

    def whole(ref, shard):
        yield ref, weight.at[pl.ds(tile(shard * rows), rows)]

    def piece(ref, row, shard, kind, last):
        yield ref.at[pl.ds(row, part)], weight.at[pl.ds(tile(shard * rows + kind * part), part)]

    copies = fetch((sources, whole, piece), scalars, own, other, buffers, sems)
    for copy in copies:
        copy.wait()
    batches = modulation.shape[0]
    tokens = middle.shape[0] // batches
    step = 2 * HEAD_DIM

    def body(i, carry):
        at = pl.ds(pl.multiple_of(i * step, step), step)
        value = jnp.dot(hidden[...], weight[:, at], preferred_element_type=jnp.float32)
        for batch in range(batches):
            span = slice(batch * tokens, (batch + 1) * tokens)
            mixed = middle[span, at].astype(jnp.float32) + modulation[batch, 5:6, at] * value[span]
            out[span, at] = mixed.astype(out.dtype)
        return carry

    lax.fori_loop(0, weight.shape[1] // step, body, 0)


def call(kernel, sources, scalars, dense, shards, buffers, outs, scratch, flops, name):
    pieces = 2 + 3 * 2 * len(sources)
    return pl.pallas_call(
        functools.partial(kernel, sources),
        out_shape=outs,
        in_specs=[pl.BlockSpec(memory_space=pltpu.SMEM)]
        + [pl.BlockSpec(memory_space=pltpu.VMEM)] * len(dense)
        + [pl.BlockSpec(memory_space=pltpu.HBM)] * (len(shards) + len(buffers)),
        out_specs=jax.tree.map(lambda _: pl.BlockSpec(memory_space=pltpu.VMEM), outs),
        scratch_shapes=[*scratch, pltpu.SemaphoreType.DMA((pieces,))],
        compiler_params=pltpu.CompilerParams(vmem_limit_bytes=40 * 2**20),
        cost_estimate=pl.CostEstimate(flops=flops, bytes_accessed=flops // 768, transcendentals=0),
        name=name,
    )(scalars, *dense, *shards, *buffers)


def routed(ring, latents, offsets, levels, mod_table, rel_bias, w_qkv, w_out, w_up, w_down):
    batches, lat_rows, columns, features = latents.shape
    inner = HEADS * HEAD_DIM
    per_dev = columns // WIN
    tokens = batches * lat_rows * columns
    group, win = lax.axis_index("groups"), lax.axis_index("win")
    z, y, core = win // (2 * ring.ys), win // 2 % ring.ys, win % 2

    def shard_of(slot, side):
        dz, dy = (slot, 0) if slot < ring.zs else (slot - ring.zs, 1)
        return ((z + ring.zs - dz) % ring.zs * ring.ys + (y + dy) % ring.ys) * 2 + (core + side) % 2

    scalars = jnp.stack(
        [shard_of(slot, side) for side in range(2) for slot in range(2 * ring.zs)] + [group]
    ).astype(jnp.int32)

    def rows_of(shard, count, parts):
        mine = lax.dynamic_slice_in_dim(shard, group * count, count, 0)
        return mine, shard[(parts - 1) * count :]

    half = w_qkv.shape[0] // 2
    values = w_qkv[:, features:]
    values = jnp.concatenate([values[:half], values[half:]], axis=1)
    keys = lax.dynamic_slice_in_dim(w_qkv[:, :features], group * half, half, 0)
    out_a, out_b = rows_of(w_out, w_out.shape[0] // 3, 3)
    third_0 = jnp.concatenate([keys, out_a, values, out_b], axis=0)
    up_a, up_b = rows_of(w_up, w_up.shape[0] // 3, 3)
    third_1 = jnp.concatenate(
        [up_a[:, :features], up_a[:, features:], up_b[:, :features], up_b[:, features:]], axis=0
    )
    down_a, down_b = rows_of(w_down, w_down.shape[0] // 3, 3)
    third_2 = jnp.concatenate([down_a, down_b], axis=0)
    early = (("r1", "y0", "r2", "y1", "x1"), ("r3", "y2", "y3", "x2", "x3", "x4"))
    late = (("r1", "y0", "r2", "y1", "x1"), ("r3", "y2", "x2"), ("y3", "x3"), ("x4",))
    with jax.named_scope("chunk0"):
        buffers_0, sources_0 = gathered(ring, third_0, early)
    swap = ring.pairs(dcore=1)
    qkv_pair, out_pair = moved(w_qkv, swap), moved(w_out, swap)
    with jax.named_scope("chunk1"):
        buffers_1, sources_1 = gathered(ring, third_1, early)
    up_pair, down_pair = moved(w_up, swap), moved(w_down, swap)
    with jax.named_scope("chunk2"):
        buffers_2, sources_2 = gathered(ring, third_2, late)

    selector = (levels[:, None] == jnp.arange(mod_table.shape[0], dtype=jnp.int32)[None, :]).astype(
        jnp.bfloat16
    )
    modulation = jnp.dot(
        selector, mod_table.reshape(mod_table.shape[0], 6 * features), preferred_element_type=jnp.float32
    ).reshape(batches, 6, features)
    wide = modulation.reshape(batches, 6, 1, 1, features)
    normed = norm_rows(latents.astype(jnp.float32)) * (1.0 + wide[:, 0]) + wide[:, 1]
    normed = normed.astype(jnp.bfloat16)
    arrived = passed_along(normed[:, :, columns - WIN :, :], "win", 1)
    widened = jnp.concatenate([arrived, normed], axis=2)
    rolled = jax.vmap(
        lambda plane, shift_by: lax.dynamic_slice_in_dim(plane, WIN - shift_by, columns, 1)
    )(widened, offsets)
    windows = rolled.reshape(batches, lat_rows, per_dev, WIN, features).transpose(0, 2, 1, 3, 4)
    windows = windows.reshape(tokens, features)
    bf16 = jnp.bfloat16
    attended = call(
        attention_kernel, sources_0, scalars, (windows, rel_bias), (w_qkv, qkv_pair), buffers_0,
        jax.ShapeDtypeStruct((tokens, inner), bf16),
        [pltpu.VMEM((features, w_qkv.shape[1]), bf16), pltpu.VMEM((tokens, w_qkv.shape[1]), bf16)],
        2 * tokens * features * w_qkv.shape[1], "attention",
    )
    attended = attended.reshape(batches, per_dev, lat_rows, WIN, inner).transpose(0, 2, 1, 3, 4)
    attended = attended.reshape(batches, lat_rows, columns, inner)
    returned = passed_along(attended[:, :, :WIN, :], "win", -1)
    restored = restore_grid(attended, returned, offsets, columns)
    flat = latents.reshape(tokens, features)
    middle, second = call(
        project_kernel, sources_0, scalars, (restored.reshape(tokens, inner), flat, modulation),
        (w_out, out_pair), buffers_0, (jax.ShapeDtypeStruct((tokens, features), bf16),) * 2,
        [pltpu.VMEM((inner, features), bf16)], 2 * tokens * inner * features, "project",
    )
    hidden = call(
        up_kernel, sources_1, scalars, (second,), (w_up, up_pair), buffers_1,
        jax.ShapeDtypeStruct((tokens, w_up.shape[1]), bf16),
        [pltpu.VMEM(((features), w_up.shape[1]), bf16)], 2 * tokens * features * w_up.shape[1], "up",
    )
    result = call(
        down_kernel, sources_2, scalars, (hidden, middle, modulation), (w_down, down_pair), buffers_2,
        jax.ShapeDtypeStruct((tokens, features), bf16),
        [pltpu.VMEM((w_up.shape[1], features), bf16)], 2 * tokens * features * w_up.shape[1], "down",
    )
    return result.reshape(latents.shape)


def solution(mesh):
    ring = Ring(mesh)

    in_specs = (
        P("groups", None, "win", None),
        P("groups"),
        P("groups"),
        P(),
        P(),
        P("win", None),
        P("win", None),
        P("win", None),
        P("win", None),
    )
    out_specs = P("groups", None, "win", None)

    def run(*args):
        body = functools.partial(routed, ring) if ring.fits(*args[5:]) else plain
        return jax.shard_map(
            body, mesh=mesh, in_specs=in_specs, out_specs=out_specs, check_vma=False
        )(*args)

    return run
```

```python
import functools

import jax
import jax.numpy as jnp
from jax import lax
from jax.experimental import pallas as pl
from jax.experimental.pallas import tpu as pltpu
from jax.sharding import PartitionSpec as P


HEADS = 6
HEAD_DIM = 128
WIN = 8
LEVELS = 32


def passed_along(shard, axis, by):
    length = lax.axis_size(axis)
    return lax.ppermute(shard, axis, [(i, (i + by) % length) for i in range(length)])


def norm_rows(values_in):
    centre = values_in - jnp.mean(values_in, axis=-1, keepdims=True)
    spread = jnp.mean(centre * centre, axis=-1, keepdims=True)
    return centre * lax.rsqrt(spread + 1e-06)


def restore_grid(region, arrived, offsets, columns):
    widened = jnp.concatenate([region, arrived], axis=2)
    return jax.vmap(lambda plane, shift_by: lax.dynamic_slice_in_dim(plane, shift_by, columns, 1))(
        widened, offsets
    )


def plain(latents, offsets, levels, mod_table, rel_bias, w_qkv, w_out, w_up, w_down):
    batches, lat_rows, columns, features = latents.shape
    inner = HEADS * HEAD_DIM
    per_dev = columns // WIN
    selector = (levels[:, None] == jnp.arange(LEVELS, dtype=jnp.int32)[None, :]).astype(
        jnp.bfloat16
    )
    modulation = jnp.dot(
        selector, mod_table.reshape(LEVELS, 6 * features), preferred_element_type=jnp.float32
    )
    modulation = modulation.reshape(batches, 6, 1, 1, features)
    stream = latents.astype(jnp.float32)
    normed = (norm_rows(stream) * (1.0 + modulation[:, 0]) + modulation[:, 1]).astype(jnp.bfloat16)
    arrived = passed_along(normed[:, :, columns - WIN :, :], "win", 1)
    widened = jnp.concatenate([arrived, normed], axis=2)
    rolled = jax.vmap(
        lambda plane, shift_by: lax.dynamic_slice_in_dim(plane, WIN - shift_by, columns, 1)
    )(widened, offsets)
    full_qkv = lax.all_gather(w_qkv, "win", axis=0, tiled=True)
    windows = rolled.reshape(batches, lat_rows, per_dev, WIN, features).transpose(0, 2, 1, 3, 4)
    windows = windows.reshape(-1, lat_rows * WIN, features)
    number = windows.shape[0]
    triple = jnp.dot(windows.reshape(-1, features), full_qkv, preferred_element_type=jnp.float32)
    triple = triple.astype(jnp.bfloat16).reshape(number, lat_rows * WIN, 3, HEADS, HEAD_DIM)
    scores = jnp.einsum(
        "wqhe,wkhe->whqk", triple[:, :, 0], triple[:, :, 1], preferred_element_type=jnp.float32
    )
    scores = scores * (1.0 / HEAD_DIM**0.5) + rel_bias[None]
    probs = jax.nn.softmax(scores, axis=-1).astype(jnp.bfloat16)
    attended = jnp.einsum(
        "whqk,wkhe->wqhe", probs, triple[:, :, 2], preferred_element_type=jnp.float32
    ).astype(jnp.bfloat16)
    attended = attended.reshape(batches, per_dev, lat_rows, WIN, inner).transpose(0, 2, 1, 3, 4)
    attended = attended.reshape(batches, lat_rows, columns, inner)
    full_out = lax.all_gather(w_out, "win", axis=0, tiled=True)
    returned = passed_along(attended[:, :, :WIN, :], "win", -1)
    restored = restore_grid(attended, returned, offsets, columns)
    projected = jnp.dot(restored.reshape(-1, inner), full_out, preferred_element_type=jnp.float32)
    projected = projected.reshape(batches, lat_rows, columns, features)
    middle = (stream + modulation[:, 2] * projected).astype(jnp.bfloat16)
    second = (
        norm_rows(middle.astype(jnp.float32)) * (1.0 + modulation[:, 3]) + modulation[:, 4]
    ).astype(jnp.bfloat16)
    full_up = lax.all_gather(w_up, "win", axis=0, tiled=True)
    hidden = jnp.dot(second.reshape(-1, features), full_up, preferred_element_type=jnp.float32)
    hidden = jax.nn.gelu(hidden, approximate=False).astype(jnp.bfloat16)
    full_down = lax.all_gather(w_down, "win", axis=0, tiled=True)
    lowered = jnp.dot(hidden, full_down, preferred_element_type=jnp.float32).reshape(
        batches, lat_rows, columns, features
    )
    return (middle.astype(jnp.float32) + modulation[:, 5] * lowered).astype(jnp.bfloat16)


AXES = ("groups", "win")


class Ring:
    def __init__(self, mesh):
        self.groups, self.length = mesh.shape["groups"], mesh.shape["win"]
        places = [tuple(d.coords) for d in mesh.devices.reshape(self.groups, self.length)[0]]
        self.ys = len({p[1] for p in places})
        self.zs = self.length // (2 * self.ys)

    def place(self, win):
        return win // (2 * self.ys), win // 2 % self.ys, win % 2

    def index(self, z, y, core):
        return (z % self.zs * self.ys + y % self.ys) * 2 + core

    def pairs(self, dx=0, dz=0, dy=0, dcore=0):
        out = []
        for group in range(self.groups):
            for win in range(self.length):
                z, y, core = self.place(win)
                target = self.index(z + dz, y + dy, (core + dcore) % 2)
                out.append((group * self.length + win, (group + dx) % self.groups * self.length + target))
        return out

    def fits(self):
        return self.groups == 2 and self.ys == 2 and self.zs == 4


def moved(block, pairs):
    return lax.ppermute(block, AXES, pairs)


SLOTS = ("own", "r1", "r2", "r3", "y0", "y1", "y2", "y3")


class Gather:
    def __init__(self, ring, name, turn):
        self.ring, self.name, self.has = ring, name, {"own": turn}

    def send(self, result, source, **by):
        self.has[result] = moved(self.has[source], self.ring.pairs(**by))

    def round_chips(self, via_z=False):
        self.send("r1", "own", dz=1)
        self.send("r3", "own", dz=-1)
        self.send("r2", "r1", dz=1)
        self.send("y0", "own", dy=1)
        if via_z:
            self.send("y1", "y0", dz=1)
        else:
            self.send("y1", "r1", dy=1)
        self.send("y2", "r2", dy=1)
        self.send("y3", "r3", dy=1)

    def across(self):
        for name in SLOTS[1:]:
            self.send("x" + name, name, dx=1)

    def buffers(self, own, crossed):
        names = SLOTS[1:]
        return [own, *(self.has[name] for name in names), *(self.has["x" + name] for name in names if crossed)]


def start_all(pairs, sems):
    copies = [pltpu.make_async_copy(src, dst, sems.at[i]) for i, (src, dst) in enumerate(pairs)]
    for copy in copies:
        copy.start()
    return copies


def halves(weight, scalars, buffers):
    rows = buffers[0].shape[0]
    half, count = rows // 2, len(SLOTS)
    yield buffers[0], weight.at[pl.ds(tile(scalars[0] * rows), rows)]
    for slot in range(1, count):
        for side, number in enumerate((slot, count - 1 + slot)):
            part = scalars[count] if side == 0 else 1 - scalars[count]
            yield (
                buffers[number],
                weight.at[pl.ds(tile(scalars[slot] * rows + part * half), half)],
            )


def blocks(weight, scalars, buffers):
    rows = buffers[0].shape[0]
    for slot, ref in enumerate(buffers):
        yield ref, weight.at[pl.ds(tile(scalars[slot] * rows), rows)]


def tile(value, by=16):
    return pl.multiple_of(value, by)


def pack_kernel(scalars, w_qkv, w_out, w_up, here, there):
    rows, inner = w_qkv.shape[0], w_out.shape[1] // 2
    width, short = inner // 2, w_out.shape[0]
    block = w_up.shape[1] // (2 * len(SLOTS))

    def pack(out, side):
        for third in range(3):
            at = third * inner + side * width
            out[:rows, third * width : (third + 1) * width] = w_qkv[:, at : at + width]
        for part in range(2):
            at = side * inner + part * width
            out[part * short : (part + 1) * short, 3 * width :] = w_out[:, at : at + width]
        for number in range(len(SLOTS)):
            at = (2 * number + side) * block
            out[rows:, number * block : (number + 1) * block] = w_up[:, at : at + block]

    core = scalars[len(SLOTS) + 1]
    for side in range(2):

        @pl.when(core == side)
        def _():
            pack(here, side)
            pack(there, 1 - side)


def join_kernel(scalars, here, there, first, narrow, up, turn):
    rows, short = here.shape[0] // 2, narrow.shape[0] // 2
    group, core = scalars[len(SLOTS)], scalars[len(SLOTS) + 1]
    wide, width = first.shape[1], here.shape[1] - first.shape[1]
    for source, side in ((here, core), (there, 1 - core)):
        at = pl.ds(tile(side * rows), rows)
        first[at, :] = source[:rows, :wide]
        up[at, :] = source[rows:, :]
        for part in range(2):
            narrow[pl.ds(tile(side * short), short), part * width : (part + 1) * width] = source[
                part * short : (part + 1) * short, wide:
            ]

        @pl.when(side == group)
        def _():
            turn[...] = source[rows:, :]


def attention_kernel(scalars, here, there, bias, *rest):
    buffers, (kept, sent, weight, triple, wide, sems) = rest[:-6], rest[-6:]
    width = kept.shape[1]
    copies = start_all(blocks(weight, scalars, buffers), sems)
    size = bias.shape[1]
    heads = width // HEAD_DIM
    first = scalars[len(SLOTS) + 1] * heads
    wide[...] = jnp.full(wide.shape, -jnp.inf, wide.dtype)
    for head in range(heads):
        for part in range(2):
            at = slice(part * size, (part + 1) * size)
            wide[head, at, at] = bias[first + head]
    for copy in copies:
        copy.wait()
    tokens = here.shape[0]
    for number, source in enumerate((here, there)):
        for third in range(3):
            at = slice(third * width, (third + 1) * width)
            triple[number * tokens : (number + 1) * tokens, at] = jnp.dot(
                source[...], weight[:, at], preferred_element_type=jnp.float32
            ).astype(triple.dtype)

    def window(i, carry):
        for number, out in enumerate((kept, sent)):
            at = pl.ds(tile(i * 2 * size), 2 * size)
            span = pl.ds(tile(number * tokens + i * 2 * size), 2 * size)
            for head in range(heads):
                cut = [
                    triple[span, third * width + head * HEAD_DIM : third * width + (head + 1) * HEAD_DIM]
                    for third in range(3)
                ]
                scores = lax.dot_general(
                    cut[0], cut[1], (((1,), (1,)), ((), ())), preferred_element_type=jnp.float32
                )
                scores = scores * (1.0 / HEAD_DIM**0.5) + wide[head]
                powers = jnp.exp(scores - jnp.max(scores, axis=-1, keepdims=True))
                probs = (powers / jnp.sum(powers, axis=-1, keepdims=True)).astype(jnp.bfloat16)
                mixed = jnp.dot(probs, cut[2], preferred_element_type=jnp.float32)
                out[at, head * HEAD_DIM : (head + 1) * HEAD_DIM] = mixed.astype(out.dtype)
        return carry

    lax.fori_loop(0, tokens // (2 * size), window, 0, unroll=True)


def bits(number):
    return number.bit_length() - 1


def one_hot(source, width):
    return jnp.where(lax.broadcasted_iota(jnp.int32, (source.shape[0], width), 1) == source, 1.0, 0.0).astype(
        jnp.bfloat16
    )


def window_kernel(offsets, levels, table, latents, strip, windows, modulation, held, stack, sems):
    batches = modulation.shape[0]
    tokens, short = latents.shape[0] // batches, strip.shape[0] // batches
    copies = start_all([(table.at[levels[i]], held.at[i]) for i in range(batches)], sems)
    for copy in copies:
        copy.wait()
    modulation[...] = held[...].astype(jnp.float32)
    lats = short // WIN
    columns = tokens // lats
    row = lax.broadcasted_iota(jnp.int32, (tokens, 1), 0)
    window, lat = row >> bits(lats * WIN), (row >> bits(WIN)) & (lats - 1)
    for batch in range(batches):
        mod = modulation[batch]
        whole, edge = slice(batch * tokens, (batch + 1) * tokens), slice(batch * short, (batch + 1) * short)
        for span, values in ((slice(tokens), latents[whole, :]), (slice(tokens, tokens + short), strip[edge, :])):
            normed = norm_rows(values.astype(jnp.float32)) * (1.0 + mod[0:1]) + mod[1:2]
            stack[span, :] = normed.astype(stack.dtype)
        place = window * WIN + (row & (WIN - 1)) + (WIN - offsets[batch])
        source = jnp.where(place < WIN, tokens + lat * WIN + place, lat * columns + place - WIN)
        taken = jnp.dot(one_hot(source, tokens + short), stack[...], preferred_element_type=jnp.float32)
        windows[whole, :] = taken.astype(windows.dtype)


def project_kernel(
    scalars, offsets, kept, back, sent, near, far, latents, modulation, w_here, w_there, middle, second, stack, taken, projected
):
    core = scalars[len(SLOTS) + 1]
    width, side_width = kept.shape[1], w_here.shape[1]
    batches = modulation.shape[0]
    tokens, short = latents.shape[0] // batches, near.shape[0] // batches
    lats = short // WIN
    columns = tokens // lats
    row = lax.broadcasted_iota(jnp.int32, (tokens, 1), 0)
    lat = row >> bits(columns)
    for batch in range(batches):
        span = slice(batch * tokens, (batch + 1) * tokens)
        edge = slice(batch * short, (batch + 1) * short)
        place = (row & (columns - 1)) + offsets[batch]
        source = jnp.where(
            place < columns,
            (((place >> bits(WIN)) * lats + lat) << bits(WIN)) + (place & (WIN - 1)),
            tokens + lat * WIN + place - columns,
        )
        stack[:tokens, :width] = kept[span, :]
        stack[:tokens, width:] = back[span, :]
        own = sent[batch * tokens : batch * tokens + short, :]
        stack[tokens:, :width] = jnp.where(core == 0, own, far[edge, :])
        stack[tokens:, width:] = near[edge, :]
        picked = jnp.dot(one_hot(source, tokens + short), stack[...], preferred_element_type=jnp.float32)
        taken[span, :] = picked.astype(taken.dtype)
    first = pl.ds(tile(core * width), width)
    last = pl.ds(tile((1 - core) * width), width)
    for number, weight in enumerate((w_here, w_there)):
        side = core if number == 0 else 1 - core
        projected[:, pl.ds(tile(side * side_width, HEAD_DIM), side_width)] = jnp.dot(
            taken[:, :width], weight[first, :], preferred_element_type=jnp.float32
        ) + jnp.dot(taken[:, width:], weight[last, :], preferred_element_type=jnp.float32)
    for batch in range(batches):
        span = slice(batch * tokens, (batch + 1) * tokens)
        mod = modulation[batch]
        mixed = latents[span, :].astype(jnp.float32) + mod[2:3] * projected[span, :]
        mixed = mixed.astype(middle.dtype)
        middle[span, :] = mixed
        normed = norm_rows(mixed.astype(jnp.float32)) * (1.0 + mod[3:4]) + mod[4:5]
        second[span, :] = normed.astype(second.dtype)


def place_kernel(places, scalars, *rest):
    buffers, (weight, sems) = rest[:-2], rest[-2:]
    for copy in start_all(places(weight, scalars, buffers), sems):
        copy.wait()


def up_kernel(scalars, here, there, weight, kept, sent):
    step = 2 * HEAD_DIM

    def body(i, carry):
        at = pl.ds(tile(i * step, step), step)
        for source, out in ((here, kept), (there, sent)):
            value = jnp.dot(source[...], weight[:, at], preferred_element_type=jnp.float32)
            value = 0.5 * value * (1.0 + lax.erf(value * 0.5**0.5))
            out[:, at] = value.astype(out.dtype)
        return carry

    lax.fori_loop(0, weight.shape[1] // step, body, 0)


def times(hidden, weight, out):
    step = 2 * HEAD_DIM

    def body(i, carry):
        at = pl.ds(tile(i * step, step), step)
        out[:, at] = jnp.dot(hidden[...], weight[:, at], preferred_element_type=jnp.float32).astype(out.dtype)
        return carry

    lax.fori_loop(0, weight.shape[1] // step, body, 0)


def down_kernel(scalars, hidden, *rest):
    buffers, (sent, weight, sems) = rest[:-3], rest[-3:]
    for copy in start_all(halves(weight, scalars, buffers), sems):
        copy.wait()
    times(hidden, weight, sent)


def lower_kernel(scalars, hidden, weight, kept):
    times(hidden, weight, kept)


def last_kernel(scalars, kept, other, middle, modulation, out):
    batches = modulation.shape[0]
    tokens = middle.shape[0] // batches
    for batch in range(batches):
        span = slice(batch * tokens, (batch + 1) * tokens)
        lowered = kept[span, :] + other[span, :].astype(jnp.float32)
        mixed = middle[span, :].astype(jnp.float32) + modulation[batch, 5:6] * lowered
        out[span, :] = mixed.astype(out.dtype)


def call(kernel, scalars, dense, pieces, outs, scratch, flops):
    copies = 5 * len(SLOTS)
    return pl.pallas_call(
        kernel,
        out_shape=outs,
        in_specs=[pl.BlockSpec(memory_space=pltpu.SMEM)]
        + [pl.BlockSpec(memory_space=pltpu.VMEM)] * len(dense)
        + [pl.BlockSpec(memory_space=pltpu.HBM)] * len(pieces),
        out_specs=jax.tree.map(lambda _: pl.BlockSpec(memory_space=pltpu.VMEM), outs),
        scratch_shapes=[*scratch, *([pltpu.SemaphoreType.DMA((copies,))] if pieces else [])],
        compiler_params=pltpu.CompilerParams(vmem_limit_bytes=32 * 2**20),
        cost_estimate=pl.CostEstimate(flops=flops, bytes_accessed=flops // 768, transcendentals=0),
    )(scalars, *dense, *pieces)


def routed(ring, latents, offsets, levels, mod_table, rel_bias, w_qkv, w_out, w_up, w_down):
    batches, lat_rows, columns, features = latents.shape
    inner = HEADS * HEAD_DIM
    tokens = batches * lat_rows * columns
    bf16, f32 = jnp.bfloat16, jnp.float32
    group, win = lax.axis_index("groups"), lax.axis_index("win")
    z, y, core = win // (2 * ring.ys), win // 2 % ring.ys, win % 2
    chips = [
        (z + ring.zs - slot % ring.zs) % ring.zs * ring.ys + (y + slot // ring.zs) % ring.ys
        for slot in range(2 * ring.zs)
    ]
    scalars = jnp.stack([*chips, group, core]).astype(jnp.int32)

    def swapped(block):
        return moved(block, ring.pairs(dcore=1))


    rows = w_qkv.shape[0]
    pack = jax.ShapeDtypeStruct((2 * rows, features), bf16)
    here, there = call(pack_kernel, scalars, (w_qkv, w_out, w_up), (), (pack,) * 2, [], 10**7)
    own, own_out, own_up, turn = call(
        join_kernel, scalars, (here, swapped(there)), (),
        (
            jax.ShapeDtypeStruct((2 * rows, 3 * inner // 2), bf16),
            jax.ShapeDtypeStruct((2 * w_out.shape[0], inner), bf16),
            pack,
            jax.ShapeDtypeStruct((rows, features), bf16),
        ),
        [], 10**7,
    )
    half = w_down.shape[0] // 2
    a, o, u = Gather(ring, "a", own), Gather(ring, "o", own_out), Gather(ring, "u", turn)
    d = Gather(ring, "d", lax.dynamic_slice_in_dim(w_down, group * half, half, 0))
    for gather in (a, o, u, d):
        gather.round_chips(via_z=gather.name in VIA_Z)
    for gather in (u, d):
        gather.across()

    flat = latents.reshape(tokens, features)
    short = batches * lat_rows * WIN
    whole = jax.ShapeDtypeStruct((tokens, features), bf16)
    vmem, smem = pl.BlockSpec(memory_space=pltpu.VMEM), pl.BlockSpec(memory_space=pltpu.SMEM)
    strip = latents[:, :, columns - WIN :, :].reshape(short, features)
    strip = passed_along(strip, "win", 1)
    stack = (tokens + short) // batches
    run = pl.pallas_call(
        window_kernel,
        out_shape=(whole, jax.ShapeDtypeStruct((batches, 6, features), f32)),
        in_specs=[smem, smem, pl.BlockSpec(memory_space=pltpu.HBM), vmem, vmem],
        out_specs=(vmem,) * 2,
        scratch_shapes=[
            pltpu.VMEM((batches, 6, features), bf16),
            pltpu.VMEM((stack, features), bf16),
            pltpu.SemaphoreType.DMA((batches,)),
        ],
        compiler_params=pltpu.CompilerParams(vmem_limit_bytes=16 * 2**20),
        cost_estimate=pl.CostEstimate(flops=10**7, bytes_accessed=10**6, transcendentals=0),
        name="norm",
    )
    windows, modulation = run(offsets, levels, mod_table, flat, strip)
    kept, sent = call(
        attention_kernel, scalars, (windows, swapped(windows), rel_bias), a.buffers(own, False),
        (jax.ShapeDtypeStruct((tokens, inner // 2), bf16),) * 2,
        [pltpu.VMEM((features, 3 * inner // 2), bf16), pltpu.VMEM((2 * tokens, 3 * inner // 2), bf16),
         pltpu.VMEM((HEADS // 2, 2 * rel_bias.shape[1], 2 * rel_bias.shape[1]), f32)],
        2 * tokens * features * w_qkv.shape[1],
    )
    out_half = call(
        functools.partial(place_kernel, blocks), scalars, (), o.buffers(own_out, False),
        jax.ShapeDtypeStruct((inner, inner), bf16), [], 10**7,
    )
    square = jax.ShapeDtypeStruct((features, features), bf16)
    loaded = call(functools.partial(place_kernel, halves), scalars, (), u.buffers(own_up, True), square, [], 10**7)
    back = swapped(sent)

    def first_window(block):
        return block.reshape(batches, -1, inner // 2)[:, : lat_rows * WIN].reshape(short, inner // 2)

    near = passed_along(first_window(kept), "win", -1)
    pairs = [(i, (i - 2) % ring.length) for i in range(ring.length) if i % 2]
    far = lax.ppermute(first_window(sent), "win", pairs)
    out_other = swapped(out_half)
    run = pl.pallas_call(
        project_kernel,
        out_shape=(whole, whole),
        in_specs=[smem, smem] + [vmem] * 9,
        out_specs=(vmem, vmem),
        scratch_shapes=[
            pltpu.VMEM((stack, inner), bf16), pltpu.VMEM((tokens, inner), bf16), pltpu.VMEM((tokens, features), f32)
        ],
        compiler_params=pltpu.CompilerParams(vmem_limit_bytes=32 * 2**20),
        cost_estimate=pl.CostEstimate(flops=2 * tokens * inner * features, bytes_accessed=10**6, transcendentals=0),
        name="project",
    )
    middle, second = run(scalars, offsets, kept, back, sent, near, far, flat, modulation, out_half, out_other)
    here, there = call(
        up_kernel, scalars, (second, swapped(second), loaded), (), (whole, whole), [],
        2 * tokens * features * w_up.shape[1],
    )
    product = tokens * features * w_up.shape[1]
    other, weight = call(
        down_kernel, scalars, (there,), d.buffers(w_down, True),
        (whole, square), [], product,
    )
    lowered = call(
        lower_kernel, scalars, (here, weight), (), jax.ShapeDtypeStruct((tokens, features), f32), [], product
    )
    result = call(last_kernel, scalars, (lowered, swapped(other), middle, modulation), (), whole, [], 10**7)
    return result.reshape(latents.shape)


VIA_Z = ("u",)


def solution(mesh):
    ring = Ring(mesh)

    in_specs = (
        P("groups", None, "win", None),
        P("groups"),
        P("groups"),
        P(),
        P(),
        P("win", None),
        P("win", None),
        P("win", None),
        P("win", None),
    )
    out_specs = P("groups", None, "win", None)

    def spread(body):
        return jax.shard_map(body, mesh=mesh, in_specs=in_specs, out_specs=out_specs, check_vma=False)

    if not ring.fits():
        return spread(plain)

    def body(*args):
        return routed(ring, *args)

    return spread(body)
```

```python
import functools

import jax
import jax.numpy as jnp
from jax import lax
from jax.experimental import pallas as pl
from jax.experimental.pallas import tpu as pltpu
from jax.sharding import PartitionSpec as P


HEADS = 6
HEAD_DIM = 128
WIN = 8
LEVELS = 32


def passed_along(shard, axis, by):
    length = lax.axis_size(axis)
    return lax.ppermute(shard, axis, [(i, (i + by) % length) for i in range(length)])


def norm_rows(values_in):
    centre = values_in - jnp.mean(values_in, axis=-1, keepdims=True)
    spread = jnp.mean(centre * centre, axis=-1, keepdims=True)
    return centre * lax.rsqrt(spread + 1e-06)


def restore_grid(region, arrived, offsets, columns):
    widened = jnp.concatenate([region, arrived], axis=2)
    return jax.vmap(lambda plane, shift_by: lax.dynamic_slice_in_dim(plane, shift_by, columns, 1))(
        widened, offsets
    )


def plain(latents, offsets, levels, mod_table, rel_bias, w_qkv, w_out, w_up, w_down):
    batches, lat_rows, columns, features = latents.shape
    inner = HEADS * HEAD_DIM
    per_dev = columns // WIN
    selector = (levels[:, None] == jnp.arange(LEVELS, dtype=jnp.int32)[None, :]).astype(
        jnp.bfloat16
    )
    modulation = jnp.dot(
        selector, mod_table.reshape(LEVELS, 6 * features), preferred_element_type=jnp.float32
    )
    modulation = modulation.reshape(batches, 6, 1, 1, features)
    stream = latents.astype(jnp.float32)
    normed = (norm_rows(stream) * (1.0 + modulation[:, 0]) + modulation[:, 1]).astype(jnp.bfloat16)
    arrived = passed_along(normed[:, :, columns - WIN :, :], "win", 1)
    widened = jnp.concatenate([arrived, normed], axis=2)
    rolled = jax.vmap(
        lambda plane, shift_by: lax.dynamic_slice_in_dim(plane, WIN - shift_by, columns, 1)
    )(widened, offsets)
    full_qkv = lax.all_gather(w_qkv, "win", axis=0, tiled=True)
    windows = rolled.reshape(batches, lat_rows, per_dev, WIN, features).transpose(0, 2, 1, 3, 4)
    windows = windows.reshape(-1, lat_rows * WIN, features)
    number = windows.shape[0]
    triple = jnp.dot(windows.reshape(-1, features), full_qkv, preferred_element_type=jnp.float32)
    triple = triple.astype(jnp.bfloat16).reshape(number, lat_rows * WIN, 3, HEADS, HEAD_DIM)
    scores = jnp.einsum(
        "wqhe,wkhe->whqk", triple[:, :, 0], triple[:, :, 1], preferred_element_type=jnp.float32
    )
    scores = scores * (1.0 / HEAD_DIM**0.5) + rel_bias[None]
    probs = jax.nn.softmax(scores, axis=-1).astype(jnp.bfloat16)
    attended = jnp.einsum(
        "whqk,wkhe->wqhe", probs, triple[:, :, 2], preferred_element_type=jnp.float32
    ).astype(jnp.bfloat16)
    attended = attended.reshape(batches, per_dev, lat_rows, WIN, inner).transpose(0, 2, 1, 3, 4)
    attended = attended.reshape(batches, lat_rows, columns, inner)
    full_out = lax.all_gather(w_out, "win", axis=0, tiled=True)
    returned = passed_along(attended[:, :, :WIN, :], "win", -1)
    restored = restore_grid(attended, returned, offsets, columns)
    projected = jnp.dot(restored.reshape(-1, inner), full_out, preferred_element_type=jnp.float32)
    projected = projected.reshape(batches, lat_rows, columns, features)
    middle = (stream + modulation[:, 2] * projected).astype(jnp.bfloat16)
    second = (
        norm_rows(middle.astype(jnp.float32)) * (1.0 + modulation[:, 3]) + modulation[:, 4]
    ).astype(jnp.bfloat16)
    full_up = lax.all_gather(w_up, "win", axis=0, tiled=True)
    hidden = jnp.dot(second.reshape(-1, features), full_up, preferred_element_type=jnp.float32)
    hidden = jax.nn.gelu(hidden, approximate=False).astype(jnp.bfloat16)
    full_down = lax.all_gather(w_down, "win", axis=0, tiled=True)
    lowered = jnp.dot(hidden, full_down, preferred_element_type=jnp.float32).reshape(
        batches, lat_rows, columns, features
    )
    return (middle.astype(jnp.float32) + modulation[:, 5] * lowered).astype(jnp.bfloat16)


AXES = ("groups", "win")


class Ring:
    def __init__(self, mesh):
        self.groups, self.length = mesh.shape["groups"], mesh.shape["win"]
        places = [tuple(d.coords) for d in mesh.devices.reshape(self.groups, self.length)[0]]
        self.ys = len({p[1] for p in places})
        self.zs = self.length // (2 * self.ys)

    def place(self, win):
        return win // (2 * self.ys), win // 2 % self.ys, win % 2

    def index(self, z, y, core):
        return (z % self.zs * self.ys + y % self.ys) * 2 + core

    def pairs(self, dx=0, dz=0, dy=0, dcore=0):
        out = []
        for group in range(self.groups):
            for win in range(self.length):
                z, y, core = self.place(win)
                target = self.index(z + dz, y + dy, (core + dcore) % 2)
                out.append((group * self.length + win, (group + dx) % self.groups * self.length + target))
        return out

    def fits(self):
        return self.groups == 2 and self.ys == 2 and self.zs == 4


def moved(block, pairs):
    return lax.ppermute(block, AXES, pairs)


SLOTS = ("own", "r1", "r2", "r3", "y0", "y1", "y2", "y3")


class Gather:
    def __init__(self, ring, name, turn):
        self.ring, self.name, self.has = ring, name, {"own": turn}

    def send(self, result, source, **by):
        self.has[result] = moved(self.has[source], self.ring.pairs(**by))

    def round_chips(self, via_z=False):
        self.send("r1", "own", dz=1)
        self.send("r3", "own", dz=-1)
        self.send("r2", "r1", dz=1)
        self.send("y0", "own", dy=1)
        if via_z:
            self.send("y1", "y0", dz=1)
        else:
            self.send("y1", "r1", dy=1)
        self.send("y2", "r2", dy=1)
        self.send("y3", "r3", dy=1)

    def across(self):
        for name in SLOTS[1:]:
            self.send("x" + name, name, dx=1)

    def pieces(self, own, crossed):
        out = [("own", 0, 0, own)]
        for slot, name in enumerate(SLOTS[1:], 1):
            out.append((name, slot, 1 if crossed else 0, self.has[name]))
            if crossed:
                out.append(("x" + name, slot, 2, self.has["x" + name]))
        return out


def start_all(pairs, sems):
    copies = [pltpu.make_async_copy(src, dst, sems.at[i]) for i, (src, dst) in enumerate(pairs)]
    for copy in copies:
        copy.start()
    return copies


def places(pieces, rows, weight, scalars, buffers):
    for (_, slot, part, _), ref in zip(pieces, buffers):
        at = scalars[slot] * rows
        if part:
            group = scalars[len(SLOTS)]
            at = at + (group if part == 1 else 1 - group) * ref.shape[0]
        yield ref, weight.at[pl.ds(tile(at), ref.shape[0])]


def tile(value, by=16):
    return pl.multiple_of(value, by)


def pack_kernel(scalars, w_qkv, w_out, w_up, here, there):
    rows, inner = w_qkv.shape[0], w_out.shape[1] // 2
    width, short = inner // 2, w_out.shape[0]
    block = w_up.shape[1] // (2 * len(SLOTS))

    def pack(out, side):
        for third in range(3):
            at = third * inner + side * width
            out[:rows, third * width : (third + 1) * width] = w_qkv[:, at : at + width]
        for part in range(2):
            at = side * inner + part * width
            out[part * short : (part + 1) * short, 3 * width :] = w_out[:, at : at + width]
        for number in range(len(SLOTS)):
            at = (2 * number + side) * block
            out[rows:, number * block : (number + 1) * block] = w_up[:, at : at + block]

    core = scalars[len(SLOTS) + 1]
    for side in range(2):

        @pl.when(core == side)
        def _():
            pack(here, side)
            pack(there, 1 - side)


def join_kernel(scalars, here, there, first, narrow, up, turn):
    rows, short = here.shape[0] // 2, narrow.shape[0] // 2
    group, core = scalars[len(SLOTS)], scalars[len(SLOTS) + 1]
    wide, width = first.shape[1], here.shape[1] - first.shape[1]
    for source, side in ((here, core), (there, 1 - core)):
        at = pl.ds(tile(side * rows), rows)
        first[at, :] = source[:rows, :wide]
        up[at, :] = source[rows:, :]
        for part in range(2):
            narrow[pl.ds(tile(side * short), short), part * width : (part + 1) * width] = source[
                part * short : (part + 1) * short, wide:
            ]

        @pl.when(side == group)
        def _():
            turn[...] = source[rows:, :]


def attention_kernel(put, scalars, here, there, bias, _, *rest):
    buffers, (kept, sent, weight, triple, wide, sems) = rest[:-6], rest[-6:]
    width = kept.shape[1]
    copies = start_all(put(weight, scalars, buffers), sems)
    size = bias.shape[1]
    heads = width // HEAD_DIM
    first = scalars[len(SLOTS) + 1] * heads
    wide[...] = jnp.full(wide.shape, -jnp.inf, wide.dtype)
    for head in range(heads):
        for part in range(2):
            at = slice(part * size, (part + 1) * size)
            wide[head, at, at] = bias[first + head]
    for copy in copies:
        copy.wait()
    tokens = here.shape[0]
    for number, source in enumerate((here, there)):
        for third in range(3):
            at = slice(third * width, (third + 1) * width)
            triple[number * tokens : (number + 1) * tokens, at] = jnp.dot(
                source[...], weight[:, at], preferred_element_type=jnp.float32
            ).astype(triple.dtype)

    def window(i, carry):
        at = pl.ds(tile(i * 2 * size), 2 * size)
        places = [(number, head) for number in range(2) for head in range(heads)]
        values, all_scores = [], []
        for number, head in places:
            span = pl.ds(tile(number * tokens + i * 2 * size), 2 * size)
            query, key, value = (
                triple[span, third * width + head * HEAD_DIM : third * width + (head + 1) * HEAD_DIM]
                for third in range(3)
            )
            scores = lax.dot_general(query, key, (((1,), (1,)), ((), ())), preferred_element_type=jnp.float32)
            all_scores.append(scores * (1.0 / HEAD_DIM**0.5) + wide[head])
            values.append(value)
        all_probs = []
        for scores in all_scores:
            powers = jnp.exp(scores - jnp.max(scores, axis=-1, keepdims=True))
            all_probs.append((powers * (1.0 / jnp.sum(powers, axis=-1, keepdims=True))).astype(jnp.bfloat16))
        for (number, head), probs, value in zip(places, all_probs, values):
            mixed = jnp.dot(probs, value, preferred_element_type=jnp.float32)
            (kept, sent)[number][at, head * HEAD_DIM : (head + 1) * HEAD_DIM] = mixed.astype(kept.dtype)
        return carry

    lax.fori_loop(0, tokens // (2 * size), window, 0, unroll=True)


def bits(number):
    return number.bit_length() - 1


def one_hot(source, width):
    return jnp.where(lax.broadcasted_iota(jnp.int32, (source.shape[0], width), 1) == source, 1.0, 0.0).astype(
        jnp.bfloat16
    )


def window_kernel(offsets, levels, table, latents, strip, windows, modulation, held, stack, sems):
    batches = modulation.shape[0]
    tokens, short = latents.shape[0] // batches, strip.shape[0] // batches
    copies = start_all([(table.at[levels[i]], held.at[i]) for i in range(batches)], sems)
    for copy in copies:
        copy.wait()
    modulation[...] = held[...].astype(jnp.float32)
    lats = short // WIN
    columns = tokens // lats
    row = lax.broadcasted_iota(jnp.int32, (tokens, 1), 0)
    window, lat = row >> bits(lats * WIN), (row >> bits(WIN)) & (lats - 1)
    for batch in range(batches):
        mod = modulation[batch]
        whole, edge = slice(batch * tokens, (batch + 1) * tokens), slice(batch * short, (batch + 1) * short)
        for span, values in ((slice(tokens), latents[whole, :]), (slice(tokens, tokens + short), strip[edge, :])):
            normed = norm_rows(values.astype(jnp.float32)) * (1.0 + mod[0:1]) + mod[1:2]
            stack[span, :] = normed.astype(stack.dtype)
        place = window * WIN + (row & (WIN - 1)) + (WIN - offsets[batch])
        source = jnp.where(place < WIN, tokens + lat * WIN + place, lat * columns + place - WIN)
        taken = jnp.dot(one_hot(source, tokens + short), stack[...], preferred_element_type=jnp.float32)
        windows[whole, :] = taken.astype(windows.dtype)


def project_kernel(
    scalars, offsets, kept, back, sent, near, far, latents, modulation, w_here, w_there, middle, second, stack, taken, projected
):
    core = scalars[len(SLOTS) + 1]
    width, side_width = kept.shape[1], w_here.shape[1]
    batches = modulation.shape[0]
    tokens, short = latents.shape[0] // batches, near.shape[0] // batches
    lats = short // WIN
    columns = tokens // lats
    row = lax.broadcasted_iota(jnp.int32, (tokens, 1), 0)
    lat = row >> bits(columns)
    for batch in range(batches):
        span = slice(batch * tokens, (batch + 1) * tokens)
        edge = slice(batch * short, (batch + 1) * short)
        place = (row & (columns - 1)) + offsets[batch]
        source = jnp.where(
            place < columns,
            (((place >> bits(WIN)) * lats + lat) << bits(WIN)) + (place & (WIN - 1)),
            tokens + lat * WIN + place - columns,
        )
        stack[:tokens, :width] = kept[span, :]
        stack[:tokens, width:] = back[span, :]
        own = sent[batch * tokens : batch * tokens + short, :]
        stack[tokens:, :width] = jnp.where(core == 0, own, far[edge, :])
        stack[tokens:, width:] = near[edge, :]
        picked = jnp.dot(one_hot(source, tokens + short), stack[...], preferred_element_type=jnp.float32)
        taken[span, :] = picked.astype(taken.dtype)
    first = pl.ds(tile(core * width), width)
    last = pl.ds(tile((1 - core) * width), width)
    for number, weight in enumerate((w_here, w_there)):
        side = core if number == 0 else 1 - core
        projected[:, pl.ds(tile(side * side_width, HEAD_DIM), side_width)] = jnp.dot(
            taken[:, :width], weight[first, :], preferred_element_type=jnp.float32
        ) + jnp.dot(taken[:, width:], weight[last, :], preferred_element_type=jnp.float32)
    for batch in range(batches):
        span = slice(batch * tokens, (batch + 1) * tokens)
        mod = modulation[batch]
        mixed = latents[span, :].astype(jnp.float32) + mod[2:3] * projected[span, :]
        mixed = mixed.astype(middle.dtype)
        middle[span, :] = mixed
        normed = norm_rows(mixed.astype(jnp.float32)) * (1.0 + mod[3:4]) + mod[4:5]
        second[span, :] = normed.astype(second.dtype)


def place_kernel(put, scalars, *rest):
    buffers, (weight, sems) = rest[:-2], rest[-2:]
    for copy in start_all(put(weight, scalars, buffers), sems):
        copy.wait()


def up_kernel(scalars, here, there, weight, kept, sent):
    step = 2 * HEAD_DIM

    def body(i, carry):
        at = pl.ds(tile(i * step, step), step)
        for source, out in ((here, kept), (there, sent)):
            value = jnp.dot(source[...], weight[:, at], preferred_element_type=jnp.float32)
            value = 0.5 * value * (1.0 + lax.erf(value * 0.5**0.5))
            out[:, at] = value.astype(out.dtype)
        return carry

    lax.fori_loop(0, weight.shape[1] // step, body, 0)


def times(hidden, weight, out):
    step = 2 * HEAD_DIM

    def body(i, carry):
        at = pl.ds(tile(i * step, step), step)
        out[:, at] = jnp.dot(hidden[...], weight[:, at], preferred_element_type=jnp.float32).astype(out.dtype)
        return carry

    lax.fori_loop(0, weight.shape[1] // step, body, 0)


def down_kernel(put, scalars, hidden, _, *rest):
    buffers, (sent, weight, sems) = rest[:-3], rest[-3:]
    for copy in start_all(put(weight, scalars, buffers), sems):
        copy.wait()
    times(hidden, weight, sent)


def lower_kernel(scalars, hidden, weight, kept):
    times(hidden, weight, kept)


def last_kernel(scalars, kept, other, middle, modulation, out):
    batches = modulation.shape[0]
    tokens = middle.shape[0] // batches
    for batch in range(batches):
        span = slice(batch * tokens, (batch + 1) * tokens)
        lowered = kept[span, :] + other[span, :].astype(jnp.float32)
        mixed = middle[span, :].astype(jnp.float32) + modulation[batch, 5:6] * lowered
        out[span, :] = mixed.astype(out.dtype)


def call(kernel, scalars, dense, pieces, outs, scratch, flops, aliases=None):
    copies = 5 * len(SLOTS)
    return pl.pallas_call(
        kernel,
        out_shape=outs,
        in_specs=[pl.BlockSpec(memory_space=pltpu.SMEM)]
        + [pl.BlockSpec(memory_space=pltpu.VMEM)] * len(dense)
        + [pl.BlockSpec(memory_space=pltpu.HBM)] * len(pieces),
        out_specs=jax.tree.map(lambda _: pl.BlockSpec(memory_space=pltpu.VMEM), outs),
        scratch_shapes=[*scratch, *([pltpu.SemaphoreType.DMA((copies,))] if pieces else [])],
        compiler_params=pltpu.CompilerParams(vmem_limit_bytes=32 * 2**20),
        cost_estimate=pl.CostEstimate(flops=flops, bytes_accessed=flops // 768, transcendentals=0),
        input_output_aliases=aliases or {},
    )(scalars, *dense, *pieces)


def placed(scalars, pieces, shape, late=()):
    rows = pieces[0][3].shape[0]
    first = [piece for piece in pieces if piece[0] not in late]
    rest = [piece for piece in pieces if piece[0] in late]
    weight = call(
        functools.partial(place_kernel, functools.partial(places, first, rows)),
        scalars, (), [piece[3] for piece in first], jax.ShapeDtypeStruct(shape, jnp.bfloat16), [], 10**7,
    )
    return weight, functools.partial(places, rest, rows), [piece[3] for piece in rest]


def routed(ring, latents, offsets, levels, mod_table, rel_bias, w_qkv, w_out, w_up, w_down):
    batches, lat_rows, columns, features = latents.shape
    inner = HEADS * HEAD_DIM
    tokens = batches * lat_rows * columns
    bf16, f32 = jnp.bfloat16, jnp.float32
    group, win = lax.axis_index("groups"), lax.axis_index("win")
    z, y, core = win // (2 * ring.ys), win // 2 % ring.ys, win % 2
    chips = [
        (z + ring.zs - slot % ring.zs) % ring.zs * ring.ys + (y + slot // ring.zs) % ring.ys
        for slot in range(2 * ring.zs)
    ]
    scalars = jnp.stack([*chips, group, core]).astype(jnp.int32)

    def swapped(block):
        return moved(block, ring.pairs(dcore=1))


    rows = w_qkv.shape[0]
    pack = jax.ShapeDtypeStruct((2 * rows, features), bf16)
    here, there = call(pack_kernel, scalars, (w_qkv, w_out, w_up), (), (pack,) * 2, [], 10**7)
    own, own_out, own_up, turn = call(
        join_kernel, scalars, (here, swapped(there)), (),
        (
            jax.ShapeDtypeStruct((2 * rows, 3 * inner // 2), bf16),
            jax.ShapeDtypeStruct((2 * w_out.shape[0], inner), bf16),
            pack,
            jax.ShapeDtypeStruct((rows, features), bf16),
        ),
        [], 10**7,
    )
    half = w_down.shape[0] // 2
    a, o, u = Gather(ring, "a", own), Gather(ring, "o", own_out), Gather(ring, "u", turn)
    d = Gather(ring, "d", lax.dynamic_slice_in_dim(w_down, group * half, half, 0))
    for gather in (a, o, u, d):
        gather.round_chips(via_z=gather.name in VIA_Z)
    for gather in (u, d):
        gather.across()

    flat = latents.reshape(tokens, features)
    short = batches * lat_rows * WIN
    whole = jax.ShapeDtypeStruct((tokens, features), bf16)
    vmem, smem = pl.BlockSpec(memory_space=pltpu.VMEM), pl.BlockSpec(memory_space=pltpu.SMEM)
    strip = latents[:, :, columns - WIN :, :].reshape(short, features)
    strip = passed_along(strip, "win", 1)
    stack = (tokens + short) // batches
    run = pl.pallas_call(
        window_kernel,
        out_shape=(whole, jax.ShapeDtypeStruct((batches, 6, features), f32)),
        in_specs=[smem, smem, pl.BlockSpec(memory_space=pltpu.HBM), vmem, vmem],
        out_specs=(vmem,) * 2,
        scratch_shapes=[
            pltpu.VMEM((batches, 6, features), bf16),
            pltpu.VMEM((stack, features), bf16),
            pltpu.SemaphoreType.DMA((batches,)),
        ],
        compiler_params=pltpu.CompilerParams(vmem_limit_bytes=16 * 2**20),
        cost_estimate=pl.CostEstimate(flops=10**7, bytes_accessed=10**6, transcendentals=0),
        name="norm",
    )
    windows, modulation = run(offsets, levels, mod_table, flat, strip)
    weight, put, late = placed(scalars, a.pieces(own, False), (features, 3 * inner // 2), LATE["a"])
    kept, sent, _ = call(
        functools.partial(attention_kernel, put), scalars,
        (windows, swapped(windows), rel_bias, weight), late,
        (*(jax.ShapeDtypeStruct((tokens, inner // 2), bf16),) * 2, jax.ShapeDtypeStruct(weight.shape, bf16)),
        [pltpu.VMEM((2 * tokens, 3 * inner // 2), bf16),
         pltpu.VMEM((HEADS // 2, 2 * rel_bias.shape[1], 2 * rel_bias.shape[1]), f32)],
        2 * tokens * features * w_qkv.shape[1], {4: 2},
    )
    out_half, _, _ = placed(scalars, o.pieces(own_out, False), (inner, inner))
    loaded, _, _ = placed(scalars, u.pieces(own_up, True), (features, features))
    square = jax.ShapeDtypeStruct((features, features), bf16)
    back = swapped(sent)

    def first_window(block):
        return block.reshape(batches, -1, inner // 2)[:, : lat_rows * WIN].reshape(short, inner // 2)

    near = passed_along(first_window(kept), "win", -1)
    pairs = [(i, (i - 2) % ring.length) for i in range(ring.length) if i % 2]
    far = lax.ppermute(first_window(sent), "win", pairs)
    out_other = swapped(out_half)
    run = pl.pallas_call(
        project_kernel,
        out_shape=(whole, whole),
        in_specs=[smem, smem] + [vmem] * 9,
        out_specs=(vmem, vmem),
        scratch_shapes=[
            pltpu.VMEM((stack, inner), bf16), pltpu.VMEM((tokens, inner), bf16), pltpu.VMEM((tokens, features), f32)
        ],
        compiler_params=pltpu.CompilerParams(vmem_limit_bytes=32 * 2**20),
        cost_estimate=pl.CostEstimate(flops=2 * tokens * inner * features, bytes_accessed=10**6, transcendentals=0),
        name="project",
    )
    middle, second = run(scalars, offsets, kept, back, sent, near, far, flat, modulation, out_half, out_other)
    here, there = call(
        up_kernel, scalars, (second, swapped(second), loaded), (), (whole, whole), [],
        2 * tokens * features * w_up.shape[1],
    )
    product = tokens * features * w_up.shape[1]
    weight, put, late = placed(scalars, d.pieces(w_down, True), (features, features), LATE["d"])
    other, weight = call(
        functools.partial(down_kernel, put), scalars, (there, weight), late,
        (whole, square), [], product, {2: 1},
    )
    lowered = call(
        lower_kernel, scalars, (here, weight), (), jax.ShapeDtypeStruct((tokens, features), f32), [], product
    )
    result = call(last_kernel, scalars, (lowered, swapped(other), middle, modulation), (), whole, [], 10**7)
    return result.reshape(latents.shape)


VIA_Z = ("u",)
LATE = {"a": ("y2", "y3"), "d": ("xr2", "y2", "xy2")}


def solution(mesh):
    ring = Ring(mesh)

    in_specs = (
        P("groups", None, "win", None),
        P("groups"),
        P("groups"),
        P(),
        P(),
        P("win", None),
        P("win", None),
        P("win", None),
        P("win", None),
    )
    out_specs = P("groups", None, "win", None)

    def spread(body):
        return jax.shard_map(body, mesh=mesh, in_specs=in_specs, out_specs=out_specs, check_vma=False)

    if not ring.fits():
        return spread(plain)

    def body(*args):
        return routed(ring, *args)

    return spread(body)
```
